32 devices in a mesh: rep: 2 (over z, core), dp: 16 (over x, y).
Axes of the slice: x: 4, y: 4, z: 1, core: 2. Of those that a mesh axis runs over, the one named last changes fastest.
The devices are a block of a 4x4x8 slice.
Arguments:
- x: bfloat16 [32, 2048, 1024], P(('rep', 'dp')), parts along dimension 0
- dy: bfloat16 [32, 2048, 1024], P(('rep', 'dp')), parts along dimension 0
- w_gate: bfloat16 [2, 1024, 3200], P(None, 'dp')
- w_up: bfloat16 [2, 1024, 3200], P(None, 'dp')
- w_down: bfloat16 [2, 3200, 1024], P(None, 'dp')
Outputs:
- output 1: bfloat16 [32, 2048, 1024], P(('rep', 'dp')), parts along dimension 0
- output 2: bfloat16 [4, 1024, 3200], P('rep', 'dp'), parts along dimension 0
- output 3: bfloat16 [4, 1024, 3200], P('rep', 'dp'), parts along dimension 0
- output 4: bfloat16 [4, 3200, 1024], P('rep', 'dp'), parts along dimension 0
There are 2 independent parts. The reference program is written for one: setup_inputs(seed, part) draws one part's arguments, and reference() takes and returns one part's arrays. A program takes and returns all parts, laid end to end along the dimension named above; an argument that names none is the same for every part.
All inputs are finite; a program needn't handle non-finite values.
Results may differ from the reference program's by a relative error of at most 0.018.
Values are sent between devices in bfloat16 or wider.
A program may use at most 768 MiB of HBM per device.

```python
import jax
import jax.numpy as jnp
from jax import lax

SEQUENCES = 16
TOKENS = 2048
D = 1024
FF = 3200
LAYERS = 2
NAMES = ("w_gate", "w_up", "w_down")
SHAPES = {"w_gate": (LAYERS, D, FF), "w_up": (LAYERS, D, FF), "w_down": (LAYERS, FF, D)}


def bump(key, n, height):
    away = (jnp.arange(n, dtype=jnp.int32) - jax.random.randint(key, (), 0, n, jnp.int32)) % n
    return jnp.where(away < n // 8, height, 1.0)


def together(key, own, strength):
    shared = jax.random.normal(key, own.shape[1:], jnp.float32)
    return (own + strength * shared) * lax.rsqrt(1 + strength * strength)


def setup_inputs(seed: int = 0, part: int = 0) -> dict:
    kx, kdy, ka, kb, kz, kf, kh, kl, *kw = jax.random.split(jax.random.key(seed), 8 + len(NAMES))
    kx, kdy, ka, kb = (jax.random.fold_in(k, part) for k in (kx, kdy, ka, kb))
    shape = (SEQUENCES, TOKENS, D)
    much_x, much_dy = jax.random.uniform(kz, (2,), jnp.float32, 0.0, 1.0)
    layers = 2.0 ** jax.random.uniform(kl, (LAYERS, 1, 1), jnp.float32, -1.0, 1.0)
    x = together(ka, jax.random.normal(kx, shape, jnp.float32), much_x) * bump(kf, D, 4.0)
    dy = together(kb, jax.random.normal(kdy, shape, jnp.float32), much_dy)
    drawn = {"x": x.astype(jnp.bfloat16), "dy": (dy * (SEQUENCES * TOKENS) ** -0.5).astype(jnp.bfloat16)}
    for key, name in zip(kw, NAMES, strict=True):
        w = jax.random.normal(key, SHAPES[name], jnp.float32) * SHAPES[name][1] ** -0.5
        drawn[name] = (w * {"w_gate": 1.0, "w_up": bump(kh, FF, 4.0), "w_down": layers}[name]).astype(jnp.bfloat16)
    return drawn


def matmul(a, w):
    return jnp.dot(a, w, preferred_element_type=jnp.float32).astype(jnp.bfloat16)


def normed(h):
    wide = h.astype(jnp.float32)
    scale = lax.rsqrt(jnp.mean(wide**2, -1, keepdims=True) + 1e-6)
    return (wide * scale).astype(jnp.bfloat16)


def layer(h, w):
    a = normed(h)
    gate = jnp.dot(a, w["w_gate"], preferred_element_type=jnp.float32)
    up = jnp.dot(a, w["w_up"], preferred_element_type=jnp.float32)
    return h + matmul((jax.nn.silu(gate) * up).astype(jnp.bfloat16), w["w_down"])


def stack(weights, h):
    return lax.scan(lambda h, w: (layer(h, w), None), h, weights)[0]


def reference(x, dy, w_gate, w_up, w_down):
    weights = dict(zip(NAMES, (w_gate, w_up, w_down), strict=True))

    def take(so_far, sequence):
        h, by_y = sequence
        _, back = jax.vjp(stack, weights, h)
        by_weights, by_h = back(by_y)
        return jax.tree.map(lambda total, term: total + term.astype(jnp.float32), so_far, by_weights), by_h

    none_yet = {name: jnp.zeros(w.shape, jnp.float32) for name, w in weights.items()}
    by_weights, by_x = lax.scan(take, none_yet, (x, dy))
    return (by_x, *(by_weights[name].astype(jnp.bfloat16) for name in NAMES))
```

```python
import jax
import jax.numpy as jnp
from jax import lax
from jax.sharding import PartitionSpec as P


NAMES = ("w_gate", "w_up", "w_down")
F32, BF16 = jnp.float32, jnp.bfloat16


def dot(a, b, ca, cb):
    return lax.dot_general(a, b, (((ca,), (cb,)), ((), ())), preferred_element_type=F32)


def normed(h):
    wide = h.astype(F32)
    scale = lax.rsqrt(jnp.mean(wide**2, -1, keepdims=True) + 1e-6)
    return (wide * scale).astype(BF16)


def gated(gate, up):
    return (jax.nn.silu(gate) * up).astype(BF16)


def after(x, *earlier):
    return lax.optimization_barrier((x, *earlier))[0]


def solution(mesh):
    groups = mesh.shape["rep"]
    swap = [(g, g ^ 1) for g in range(groups)]

    def step(x, dy, w_gate, w_up, w_down):
        layers = w_gate.shape[0]
        first = lax.rem(lax.axis_index("rep"), 2) == 0
        x, dy = x[0], dy[0]

        def exchanged(own):
            return lax.ppermute(own, "rep", swap)

        def gather(block):
            return lax.all_gather(block, "dp", axis=0, tiled=True)

        def scatter(term):
            return lax.psum_scatter(term, "dp", scatter_dimension=0, tiled=True)

        half = w_down.shape[2] // 2
        owns, own_downs = [], []
        for n in range(layers):
            owns.append(gather(jnp.where(first, w_gate[n], w_up[n])))
            own_downs.append(gather(jnp.where(first, w_down[n, :, :half], w_down[n, :, half:])))

        h, kept, pair, down = x, [], [], []
        for n in range(layers):
            a = normed(h)
            own = after(owns[n], a)
            pair.append((own, exchanged(own)))
            one = dot(a, own, 1, 0)
            own_down = after(own_downs[n], one)
            other = exchanged(own_down)
            down.append(
                jnp.where(first, jnp.concatenate([own_down, other], 1), jnp.concatenate([other, own_down], 1))
            )
            two = dot(a, pair[n][1], 1, 0)
            act = gated(jnp.where(first, one, two), jnp.where(first, two, one))
            kept.append((h, a, one, two, act))
            if n + 1 < layers:
                h = h + dot(act, down[n], 1, 0).astype(BF16)

        by_h, sums, by_w = dy, {}, []
        for n in reversed(range(layers)):
            h, a, one, two, act = kept[n]
            by_down = dot(act, by_h, 0, 0).astype(BF16)
            by_down, by_h_then = lax.optimization_barrier((by_down, by_h))
            sums["w_down", n] = scatter(after(by_down, *by_w))
            by_act = dot(by_h_then, down[n], 1, 1).astype(BF16)
            gate, up = jnp.where(first, one, two), jnp.where(first, two, one)
            _, back = jax.vjp(gated, gate, up)
            by_gate, by_up = back(by_act)
            by_one = jnp.where(first, by_gate, by_up).astype(BF16)
            by_two = jnp.where(first, by_up, by_gate).astype(BF16)
            terms = [dot(a, t, 0, 0).astype(BF16) for t in (by_one, by_two)]
            by_one, by_two, *_ = lax.optimization_barrier((by_one, by_two, *terms))
            by_w = [scatter(after(t, sums["w_down", n])) for t in terms]
            sums["w_gate", n] = jnp.where(first, by_w[0], by_w[1])
            sums["w_up", n] = jnp.where(first, by_w[1], by_w[0])
            by_a = dot(by_one, pair[n][0], 1, 1).astype(BF16) + dot(by_two, pair[n][1], 1, 1).astype(BF16)
            _, back = jax.vjp(normed, h)
            by_h = by_h + back(by_a)[0]

        return (by_h[None], *(jnp.stack([sums[name, n] for n in range(layers)]) for name in NAMES))

    rows = P(None, "dp", None)
    tokens = P(("rep", "dp"), None, None)
    return jax.shard_map(
        step,
        mesh=mesh,
        in_specs=(tokens, tokens, rows, rows, rows),
        out_specs=(tokens, *(P("rep", "dp", None),) * 3),
        check_vma=False,
    )
```
